32 devices in a mesh: gz: 8 (over z, y), gy: 4 (over x, core).
Axes of the slice: x: 2, y: 2, z: 4, core: 2. Of those that a mesh axis runs over, the one named last changes fastest.
Arguments:
- charges: float32 [64, 64, 1024], P('gz', 'gy'), may hold values from -6 to 6
- kernel: float32 [64, 64, 64], P('gz', 'gy'), may hold values from -0.01171875 to 0.01171875
Outputs:
- fine_potential: float32 [128, 128, 2048], P('gz', 'gy')
The draws below stay inside these ranges and needn't reach their ends.
All inputs are finite; a program needn't handle non-finite values.
Results may differ from the reference program's by a relative error of at most 0.000098.
Values sent between devices are 32-bit elements; how exact they have to be, the bound alone decides.
A program may use at most 128 MiB of HBM per device.

```python
import jax
import jax.numpy as jnp

GRID = 64
REPL = 16
FINE = 128


def block_scale(own_key, shape, cuts, smallest, largest):
    gain = 1.0
    for position, parts in cuts:
        steps = jax.random.uniform(jax.random.fold_in(jax.random.fold_in(own_key, 6), position), (parts,), jnp.float32, smallest / len(cuts), largest / len(cuts))
        gain = gain * jnp.repeat(jnp.exp(steps), shape[position] // parts).reshape((-1,) + (1,) * (len(shape) - 1 - position))
    return gain


def bell_draw(key, shape, width, bound, split=(), held_as=jnp.bfloat16):
    values = jax.random.normal(key, shape, jnp.float32) * width
    if len(split) > 0:
        values = block_scale(key, shape, split, -0.22, 0.18) * values
    return jnp.clip(values, min=-bound, max=bound).astype(held_as)


def setup_inputs(seed: int = 0) -> dict:
    streams_of = jax.random.split(jax.random.key(seed), 3)
    charges = bell_draw(streams_of[0], (GRID, GRID, GRID * REPL), 1.0, 6.0, ((0, 8), (1, 4)), jnp.float32)
    kernel = bell_draw(streams_of[1], (GRID, GRID, GRID), (GRID * GRID * GRID) ** -0.5, 0.01171875, ((0, 8), (1, 4)), jnp.float32)
    return {"charges": charges, "kernel": kernel}


def refine(coarse, axis):
    before = jnp.roll(coarse, 1, axis)
    after = jnp.roll(coarse, -1, axis)
    after_two = jnp.roll(coarse, -2, axis)
    middle = (9.0 * (coarse + after) - (before + after_two)) / 16.0
    stacked = jnp.stack([coarse, middle], axis=axis + 1)
    shape = list(coarse.shape)
    shape[axis] = 2 * shape[axis]
    return stacked.reshape(shape)


def reference(charges, kernel):
    grids = charges.reshape(GRID, GRID, GRID, REPL)
    charge_spec = jnp.fft.fftn(grids, axes=(0, 1, 2))
    kernel_spec = jnp.fft.fftn(kernel, axes=(0, 1, 2))
    potential = jnp.fft.ifftn(charge_spec * kernel_spec[:, :, :, None], axes=(0, 1, 2)).real.astype(jnp.float32)
    result = refine(potential, 0)
    result = refine(result, 1)
    result = refine(result, 2)
    return result.reshape(FINE, FINE, FINE * REPL)
```

```python
import math

import jax
import jax.numpy as jnp
import numpy as np
from jax import lax
from jax.sharding import PartitionSpec as P

AXES = ("gz", "gy")


def angle(first, second, count):
    return 2.0 * np.pi / count * ((first * second) % count)


def x_table(count, replicas, devices):
    half = replicas // 2
    columns = count * half // devices
    device, part, column, x, side, pair = np.ix_(
        *(np.arange(s) for s in (devices, 2, columns, count, 2, half))
    )
    flat = device * columns + column
    theta = angle(flat // half, x, count)
    value = np.where(part == side, np.cos(theta), np.where(part == 0, np.sin(theta), -np.sin(theta)))
    value = value * (flat % half == pair)
    return value.reshape(devices * 2 * columns, count, replicas)


def x_kernel_table(count, replicas, devices):
    half = replicas // 2
    columns = count * half // devices
    lines = max(1, columns // half)
    device, part, line, x = np.ix_(*(np.arange(s) for s in (devices, 2, lines, count)))
    theta = angle(device * columns // half + line, x, count)
    value = np.where(part == 0, np.cos(theta), -np.sin(theta))
    return value.reshape(devices * 2 * lines, count)


def y_table(count, planes, rows):
    part, block, plane, row, new_plane, new_part, freq = np.ix_(
        *(np.arange(s) for s in (2, count // rows, planes, rows, planes, 2, count))
    )
    theta = angle(block * rows + row, freq, count)
    value = np.where(
        part == new_part, np.cos(theta), np.where(new_part == 0, np.sin(theta), -np.sin(theta))
    )
    value = value * (plane == new_plane)
    return value.reshape(2 * count * planes, planes * 2 * count)


def z_table(count, planes, columns, lines, group, wave):
    blocks = count // planes
    low, high, column, z_low, z_high, line = np.ix_(
        *(np.arange(s) for s in (planes, blocks, columns, planes, blocks, lines))
    )
    theta = angle(high * planes + low, z_high * planes + z_low, count)
    value = wave(theta) * (column // group == line)
    return value.reshape(count * columns, count * lines)


def refined(values, axis):
    before = np.roll(values, 1, axis)
    after = np.roll(values, -1, axis)
    after_two = np.roll(values, -2, axis)
    middle = (9.0 * (values + after) - (before + after_two)) / 16.0
    stacked = np.stack([values, middle], axis=axis + 1)
    shape = list(values.shape)
    shape[axis] = 2 * shape[axis]
    return stacked.reshape(shape)


def const(values):
    return jnp.asarray(np.asarray(values, np.float32))


def dot(left, right, dims=((1,), (0,))):
    return lax.dot_general(
        left, right, (dims, ((), ())), precision=lax.Precision.HIGH,
        preferred_element_type=jnp.float32,
    )


def extended(block, axis, dim):
    size = lax.axis_size(axis)
    forward = [(i, (i + 1) % size) for i in range(size)]
    backward = [(target, source) for source, target in forward]
    low = lax.ppermute(lax.slice_in_dim(block, block.shape[dim] - 1, None, axis=dim), axis, forward)
    high = lax.ppermute(lax.slice_in_dim(block, 0, 2, axis=dim), axis, backward)
    return jnp.concatenate([low, block, high], axis=dim)


def refine_rim(haloed, axis, count):
    centre = lax.slice_in_dim(haloed, 1, 1 + count, axis=axis)
    before = lax.slice_in_dim(haloed, 0, count, axis=axis)
    after = lax.slice_in_dim(haloed, 2, 2 + count, axis=axis)
    after_two = lax.slice_in_dim(haloed, 3, 3 + count, axis=axis)
    middle = (9.0 * (centre + after) - (before + after_two)) / 16.0
    stacked = jnp.stack([centre, middle], axis=axis + 1)
    shape = list(centre.shape)
    shape[axis] = 2 * count
    return stacked.reshape(shape)


def per_device(charges, kernel):
    planes, rows, count = kernel.shape
    replicas = charges.shape[2] // count
    half = replicas // 2
    blocks_z, blocks_y = lax.axis_size("gz"), lax.axis_size("gy")
    devices = blocks_z * blocks_y
    place = planes * rows
    columns = count * half // devices
    lines = max(1, columns // half)
    table_x = x_table(count, replicas, devices)
    table_y = const(y_table(count, planes, rows))
    cos_z = const(z_table(count, planes, columns, columns, 1, np.cos))
    sin_z = const(z_table(count, planes, columns, columns, 1, np.sin))
    cos_k = const(z_table(count, planes, columns, lines, half, np.cos) / count**3)
    sin_k = const(z_table(count, planes, columns, lines, half, np.sin) / count**3)

    sent = dot(const(table_x.reshape(-1, count * replicas)), charges.reshape(place, -1), ((1,), (1,)))
    sent_k = dot(const(x_kernel_table(count, replicas, devices)), kernel.reshape(place, count), ((1,), (1,)))
    both = jnp.concatenate(
        [sent.reshape(devices, 2 * columns, place), sent_k.reshape(devices, 2 * lines, place)], axis=1
    )
    both = lax.all_to_all(both, AXES, split_axis=0, concat_axis=0, tiled=True)

    def by_y(block, width):
        block = block.reshape(blocks_z, blocks_y, 2, width, place).transpose(0, 3, 2, 1, 4)
        block = dot(block.reshape(blocks_z * width, 2 * blocks_y * place), table_y)
        block = block.reshape(blocks_z * width, planes, 2 * count).transpose(1, 0, 2)
        return block.reshape(count * width, 2 * count)

    def swap(values):
        return jnp.concatenate([values[:, count:], values[:, :count]], axis=1)

    sign = jnp.where(lax.broadcasted_iota(jnp.int32, (1, 2 * count), 1) < count, 1.0, -1.0)
    data = by_y(both[:, : 2 * columns], columns)
    green = by_y(both[:, 2 * columns :], lines)
    data = dot(cos_z, data) + sign * swap(dot(sin_z, data))
    green = dot(cos_k, green) + sign * swap(dot(sin_k, green))
    real, imag = green[:, :count], green[:, count:]
    data = data * jnp.concatenate([real, real], axis=1) + swap(data) * jnp.concatenate([-imag, imag], axis=1)
    data = dot(cos_z, data) - sign * swap(dot(sin_z, data))
    data = data.reshape(planes, blocks_z * columns, 2 * count).transpose(1, 0, 2)
    data = dot(data.reshape(blocks_z * columns, planes * 2 * count), table_y, ((1,), (1,)))
    data = data.reshape(blocks_z, columns, 2, blocks_y, place).transpose(0, 3, 2, 1, 4)
    data = lax.all_to_all(
        data.reshape(devices, 2 * columns, place), AXES, split_axis=0, concat_axis=0, tiled=True
    )
    fine_x = const(refined(table_x, 1).reshape(-1, 2 * count * replicas))
    result = dot(data.reshape(devices * 2 * columns, place), fine_x, ((0,), (0,)))
    result = result.reshape(planes, rows, 2 * count * replicas)
    result = extended(extended(result, "gz", 0), "gy", 1)
    result = refine_rim(result, 0, planes)
    return refine_rim(result, 1, rows)


def solution(mesh):
    placed = (P("gz", "gy", None), P("gz", "gy", None))
    return jax.shard_map(
        per_device, mesh=mesh, in_specs=placed, out_specs=P("gz", "gy", None), check_vma=False
    )
```

```python
import functools

import jax
import jax.numpy as jnp
import numpy as np
from jax import lax
from jax.experimental import pallas as pl
from jax.experimental.pallas import tpu as pltpu
from jax.sharding import PartitionSpec as P

AXES = ("gz", "gy")


def angle(first, second, count):
    return 2.0 * np.pi / count * ((first * second) % count)


def x_table(count, replicas, devices):
    half = replicas // 2
    columns = count * half // devices
    device, part, column, x, side, pair = np.ix_(
        *(np.arange(s) for s in (devices, 2, columns, count, 2, half))
    )
    flat = device * columns + column
    theta = angle(flat // half, x, count)
    value = np.where(part == side, np.cos(theta), np.where(part == 0, np.sin(theta), -np.sin(theta)))
    value = value * (flat % half == pair)
    return value.reshape(devices * 2 * columns, count, replicas)


def x_kernel_table(count, replicas, devices):
    half = replicas // 2
    columns = count * half // devices
    lines = max(1, columns // half)
    device, part, line, x = np.ix_(*(np.arange(s) for s in (devices, 2, lines, count)))
    theta = angle(device * columns // half + line, x, count)
    value = np.where(part == 0, np.cos(theta), -np.sin(theta))
    return value.reshape(devices * 2 * lines, count)


def y_table(count, planes, rows):
    part, block, plane, row, new_plane, new_part, freq = np.ix_(
        *(np.arange(s) for s in (2, count // rows, planes, rows, planes, 2, count))
    )
    theta = angle(block * rows + row, freq, count)
    value = np.where(
        part == new_part, np.cos(theta), np.where(new_part == 0, np.sin(theta), -np.sin(theta))
    )
    value = value * (plane == new_plane)
    return value.reshape(2 * count * planes, planes * 2 * count)


def z_table(count, planes, columns, lines, group, wave):
    blocks = count // planes
    low, high, column, z_low, z_high, line = np.ix_(
        *(np.arange(s) for s in (planes, blocks, columns, planes, blocks, lines))
    )
    theta = angle(high * planes + low, z_high * planes + z_low, count)
    value = wave(theta) * (column // group == line)
    return value.reshape(count * columns, count * lines)


def refined(values, axis):
    before = np.roll(values, 1, axis)
    after = np.roll(values, -1, axis)
    after_two = np.roll(values, -2, axis)
    middle = (9.0 * (values + after) - (before + after_two)) / 16.0
    stacked = np.stack([values, middle], axis=axis + 1)
    shape = list(values.shape)
    shape[axis] = 2 * shape[axis]
    return stacked.reshape(shape)


def const(values):
    return jnp.asarray(np.asarray(values, np.float32))


def dot(left, right, dims=((1,), (0,))):
    return lax.dot_general(
        left, right, (dims, ((), ())), precision=lax.Precision.HIGH,
        preferred_element_type=jnp.float32,
    )


def extended(block, axis, dim):
    size = lax.axis_size(axis)
    forward = [(i, (i + 1) % size) for i in range(size)]
    backward = [(target, source) for source, target in forward]
    low = lax.ppermute(lax.slice_in_dim(block, block.shape[dim] - 1, None, axis=dim), axis, forward)
    high = lax.ppermute(lax.slice_in_dim(block, 0, 2, axis=dim), axis, backward)
    return jnp.concatenate([low, block, high], axis=dim)


def refine_rim(haloed, axis, count):
    centre = lax.slice_in_dim(haloed, 1, 1 + count, axis=axis)
    before = lax.slice_in_dim(haloed, 0, count, axis=axis)
    after = lax.slice_in_dim(haloed, 2, 2 + count, axis=axis)
    after_two = lax.slice_in_dim(haloed, 3, 3 + count, axis=axis)
    middle = (9.0 * (centre + after) - (before + after_two)) / 16.0
    stacked = jnp.stack([centre, middle], axis=axis + 1)
    shape = list(centre.shape)
    shape[axis] = 2 * count
    return stacked.reshape(shape)


def plain(charges, kernel):
    planes, rows, count = kernel.shape
    replicas = charges.shape[2] // count
    half = replicas // 2
    blocks_z, blocks_y = lax.axis_size("gz"), lax.axis_size("gy")
    devices = blocks_z * blocks_y
    place = planes * rows
    columns = count * half // devices
    lines = max(1, columns // half)
    table_x = x_table(count, replicas, devices)
    table_y = const(y_table(count, planes, rows))
    cos_z = const(z_table(count, planes, columns, columns, 1, np.cos))
    sin_z = const(z_table(count, planes, columns, columns, 1, np.sin))
    cos_k = const(z_table(count, planes, columns, lines, half, np.cos) / count**3)
    sin_k = const(z_table(count, planes, columns, lines, half, np.sin) / count**3)

    sent = dot(const(table_x.reshape(-1, count * replicas)), charges.reshape(place, -1), ((1,), (1,)))
    sent_k = dot(const(x_kernel_table(count, replicas, devices)), kernel.reshape(place, count), ((1,), (1,)))
    both = jnp.concatenate(
        [sent.reshape(devices, 2 * columns, place), sent_k.reshape(devices, 2 * lines, place)], axis=1
    )
    both = lax.all_to_all(both, AXES, split_axis=0, concat_axis=0, tiled=True)

    def by_y(block, width):
        block = block.reshape(blocks_z, blocks_y, 2, width, place).transpose(0, 3, 2, 1, 4)
        block = dot(block.reshape(blocks_z * width, 2 * blocks_y * place), table_y)
        block = block.reshape(blocks_z * width, planes, 2 * count).transpose(1, 0, 2)
        return block.reshape(count * width, 2 * count)

    def swap(values):
        return jnp.concatenate([values[:, count:], values[:, :count]], axis=1)

    sign = jnp.where(lax.broadcasted_iota(jnp.int32, (1, 2 * count), 1) < count, 1.0, -1.0)
    data = by_y(both[:, : 2 * columns], columns)
    green = by_y(both[:, 2 * columns :], lines)
    data = dot(cos_z, data) + sign * swap(dot(sin_z, data))
    green = dot(cos_k, green) + sign * swap(dot(sin_k, green))
    real, imag = green[:, :count], green[:, count:]
    data = data * jnp.concatenate([real, real], axis=1) + swap(data) * jnp.concatenate([-imag, imag], axis=1)
    data = dot(cos_z, data) - sign * swap(dot(sin_z, data))
    data = data.reshape(planes, blocks_z * columns, 2 * count).transpose(1, 0, 2)
    data = dot(data.reshape(blocks_z * columns, planes * 2 * count), table_y, ((1,), (1,)))
    data = data.reshape(blocks_z, columns, 2, blocks_y, place).transpose(0, 3, 2, 1, 4)
    data = lax.all_to_all(
        data.reshape(devices, 2 * columns, place), AXES, split_axis=0, concat_axis=0, tiled=True
    )
    fine_x = const(refined(table_x, 1).reshape(-1, 2 * count * replicas))
    result = dot(data.reshape(devices * 2 * columns, place), fine_x, ((0,), (0,)))
    result = result.reshape(planes, rows, 2 * count * replicas)
    result = extended(extended(result, "gz", 0), "gy", 1)
    result = refine_rim(result, 0, planes)
    return refine_rim(result, 1, rows)


LANES = 128
MESH = pl.DeviceIdType.MESH


def table(values):
    high = np.asarray(values, np.float32).astype(jnp.bfloat16)
    low = (np.asarray(values, np.float64) - high.astype(np.float64)).astype(jnp.bfloat16)
    return [jnp.asarray(high), jnp.asarray(low)]


def split(values):
    high = values.astype(jnp.bfloat16)
    return high, (values - high.astype(jnp.float32)).astype(jnp.bfloat16)


def mul(left, right, dims=((1,), (0,))):
    return lax.dot_general(left, right, (dims, ((), ())), preferred_element_type=jnp.float32)


def mul3(left, right, dims=((1,), (0,))):
    (a, b), (c, d) = left, right
    return mul(a, d, dims) + mul(b, c, dims) + mul(a, c, dims)


def call(body, out_shape, *operands):
    return pl.pallas_call(
        body,
        out_shape=jax.ShapeDtypeStruct(out_shape, jnp.float32),
        in_specs=[pl.BlockSpec(memory_space=pltpu.VMEM)] * len(operands),
        out_specs=pl.BlockSpec(memory_space=pltpu.VMEM),
        compiler_params=pltpu.CompilerParams(vmem_limit_bytes=60 * 1024 * 1024),
    )(*operands)


def exchange_kernel(blocks_z, blocks_y, x_ref, o_ref, send_sem, recv_sem, own_sem):
    devices = blocks_z * blocks_y
    me = lax.axis_index("gz") * blocks_y + lax.axis_index("gy")

    def partner(step):
        other = lax.rem(me + step, devices)
        return other, (other // blocks_y, lax.rem(other, blocks_y))

    barrier = pltpu.get_barrier_semaphore()
    for step in range(1, devices):
        pl.semaphore_signal(barrier, inc=1, device_id=partner(step)[1], device_id_type=MESH)
    own = pltpu.make_async_copy(x_ref.at[me], o_ref.at[me], own_sem)
    own.start()
    pl.semaphore_wait(barrier, devices - 1)
    copies = []
    for step in range(1, devices):
        other, place = partner(step)
        copy = pltpu.make_async_remote_copy(
            src_ref=x_ref.at[other], dst_ref=o_ref.at[me],
            send_sem=send_sem.at[step], recv_sem=recv_sem.at[step],
            device_id=place, device_id_type=MESH,
        )
        copy.start()
        copies.append(copy)
    for copy in copies:
        copy.wait()
    own.wait()


def exchange(blocks, blocks_z, blocks_y, number):
    devices = blocks_z * blocks_y
    return pl.pallas_call(
        functools.partial(exchange_kernel, blocks_z, blocks_y),
        out_shape=jax.ShapeDtypeStruct(blocks.shape, blocks.dtype),
        in_specs=[pl.BlockSpec(memory_space=pltpu.VMEM)],
        out_specs=pl.BlockSpec(memory_space=pltpu.VMEM),
        scratch_shapes=[
            pltpu.SemaphoreType.DMA((devices,)),
            pltpu.SemaphoreType.DMA((devices,)),
            pltpu.SemaphoreType.DMA,
        ],
        compiler_params=pltpu.CompilerParams(collective_id=number, has_side_effects=True),
    )(blocks)


def first_kernel(width, q_ref, k_ref, wh, wl, kh, kl, o_ref):
    devices = o_ref.shape[0]
    dims = ((1,), (1,))
    sent = mul3((wh[...], wl[...]), split(q_ref[...]), dims)
    o_ref[:, :width, :] = sent.reshape(devices, width, LANES)
    sent = mul3((kh[...], kl[...]), split(k_ref[...]), dims)
    o_ref[:, width:, :] = sent.reshape(devices, 8, LANES)


def middle_kernel(columns, count, x_ref, yh, yl, ch, cl, sh, sl, ah, al, bh, bl, o_ref):
    blocks_z, blocks_y = o_ref.shape[0], o_ref.shape[1]
    planes = count // blocks_z
    table_y = (yh[...], yl[...])
    cos_z, sin_z = (ch[...], cl[...]), (sh[...], sl[...])
    lane = lax.broadcasted_iota(jnp.int32, (1, LANES), 1)
    sign = jnp.where(lane < count, 1.0, -1.0)

    def swap(values):
        return pltpu.roll(values, count, 1)

    def lines_first(values):
        return jnp.concatenate([values[:, p * LANES : (p + 1) * LANES] for p in range(planes)], axis=0)

    data = jnp.concatenate(
        [
            x_ref[:, y, c * columns : (c + 1) * columns, :].reshape(blocks_z * columns, LANES)
            for c in range(2)
            for y in range(blocks_y)
        ],
        axis=1,
    )
    green = jnp.concatenate(
        [x_ref[:, y, 2 * columns :, :].reshape(blocks_z * 8, LANES) for y in range(blocks_y)], axis=1
    )
    data = lines_first(mul3(split(data), table_y))
    deep = blocks_y * LANES
    green = lines_first(mul3(split(green), (yh[:deep, :], yl[:deep, :])))
    data = split(data)
    data = mul3(cos_z, data) + sign * swap(mul3(sin_z, data))
    green = split(green)
    green = mul3((ah[...], al[...]), green) - sign * swap(mul3((bh[...], bl[...]), green))
    other = swap(green)
    real = jnp.where(lane < count, green, other)
    imag = jnp.where(lane < count, -other, green)
    data = split(data * real + swap(data) * imag)
    data = mul3(cos_z, data) - sign * swap(mul3(sin_z, data))
    size = blocks_z * columns
    data = jnp.concatenate([data[p * size : (p + 1) * size, :] for p in range(planes)], axis=1)
    data = mul3(split(data), table_y, ((1,), (1,)))
    for c in range(2):
        for y in range(blocks_y):
            start = (c * blocks_y + y) * LANES
            o_ref[:, y, c * columns : (c + 1) * columns, :] = data[:, start : start + LANES].reshape(
                blocks_z, columns, LANES
            )


def last_kernel(x_ref, wh, wl, o_ref):
    turned = jnp.transpose(x_ref[...])
    o_ref[...] = mul3(split(turned), (wh[...], wl[...]))


def refine_kernel(x_ref, r_ref, t_ref, o_ref):
    step = pl.program_id(0)
    near = x_ref[pl.ds(step, 4)].reshape(4 * x_ref.shape[1], x_ref.shape[2])
    high, low = split(near)
    fine = mul(r_ref[...], low) + mul(r_ref[...], high)
    high, low = split(fine)
    blocks = fine.shape[1] // LANES
    for b in range(blocks):
        def window(values):
            pieces = [(b + s) % blocks * LANES for s in (-1, 0, 1)]
            return jnp.concatenate([values[:, p : p + LANES] for p in pieces], axis=1)

        made = mul(window(low), t_ref[...]) + mul(window(high), t_ref[...])
        o_ref[:, :, 2 * b * LANES : 2 * (b + 1) * LANES] = made.reshape(2, -1, 2 * LANES)


def rim_table(count):
    made = np.zeros((2 * count, count + 3))
    for i in range(count):
        made[2 * i, i + 1] = 1.0
        made[2 * i + 1, i : i + 4] = np.array([-1.0, 9.0, 9.0, -1.0]) / 16.0
    return made


def refine(coarse, planes, rows, width, replicas):
    haloed = extended(extended(coarse, "gz", 0), "gy", 1)
    deep = -(-(rows + 3) // 8) * 8
    haloed = jnp.pad(haloed, ((0, 0), (0, deep - rows - 3), (0, 0)))
    along_y = np.pad(rim_table(rows), ((0, 0), (0, deep - rows - 3)))
    both = jnp.asarray(np.kron(rim_table(1), along_y), jnp.bfloat16)
    count = width // replicas
    spread = refined(np.eye(width).reshape(width, count, replicas), 1).reshape(width, 2 * width)
    spread = jnp.asarray(spread[: 3 * LANES, 2 * LANES : 4 * LANES], jnp.bfloat16)
    return pl.pallas_call(
        refine_kernel,
        grid=(planes,),
        out_shape=jax.ShapeDtypeStruct((2 * planes, 2 * rows, 2 * width), jnp.float32),
        in_specs=[
            pl.BlockSpec(haloed.shape, lambda i: (0, 0, 0)),
            pl.BlockSpec(both.shape, lambda i: (0, 0)),
            pl.BlockSpec(spread.shape, lambda i: (0, 0)),
        ],
        out_specs=pl.BlockSpec((2, 2 * rows, 2 * width), lambda i: (i, 0, 0)),
    )(haloed, both, spread)


def z_green_table(count, planes, columns, group, first, second):
    lines = max(1, columns // group)
    rows = []
    for wave in (first, second):
        made = z_table(count, planes, columns, lines, group, wave)
        rows.append(made.reshape(count * columns, count, lines))
    made = np.concatenate(rows, axis=2)
    made = np.pad(made, ((0, 0), (0, 0), (0, 8 - 2 * lines)))
    return made.reshape(count * columns, count * 8)


def per_device(charges, kernel):
    planes, rows, count = kernel.shape
    width = charges.shape[2]
    replicas = width // count
    half = replicas // 2
    blocks_z, blocks_y = lax.axis_size("gz"), lax.axis_size("gy")
    devices = blocks_z * blocks_y
    place = planes * rows
    columns = count * half // devices
    lines = max(1, columns // half)
    fits = place == LANES and 2 * count == LANES and columns % 8 == 0 and 2 * lines <= 8
    if not fits or LANES % replicas or width < 3 * LANES:
        return plain(charges, kernel)
    table_x = table(x_table(count, replicas, devices).reshape(-1, width))
    lines_x = x_kernel_table(count, replicas, devices).reshape(devices, 2 * lines, count)
    lines_x = table(np.pad(lines_x, ((0, 0), (0, 8 - 2 * lines), (0, 0))).reshape(devices * 8, count))
    table_y = table(y_table(count, planes, rows))
    cos_z = table(z_table(count, planes, columns, columns, 1, np.cos))
    sin_z = table(z_table(count, planes, columns, columns, 1, np.sin))
    scale = 1.0 / count**3
    green_a = table(scale * z_green_table(count, planes, columns, half, np.cos, np.sin))
    green_b = table(scale * z_green_table(count, planes, columns, half, lambda t: -np.sin(t), np.cos))

    sent = call(
        functools.partial(first_kernel, 2 * columns), (devices, 2 * columns + 8, LANES),
        charges.reshape(place, width), kernel.reshape(place, count), *table_x, *lines_x,
    )
    held = exchange(sent, blocks_z, blocks_y, 0)
    sent = call(
        functools.partial(middle_kernel, columns, count), (blocks_z, blocks_y, 2 * columns, LANES),
        held.reshape(blocks_z, blocks_y, 2 * columns + 8, LANES),
        *table_y, *cos_z, *sin_z, *green_a, *green_b,
    )
    held = exchange(sent.reshape(devices, 2 * columns, LANES), blocks_z, blocks_y, 1)
    coarse = call(last_kernel, (place, width), held.reshape(width, LANES), *table_x)
    return refine(coarse.reshape(planes, rows, width), planes, rows, width, replicas)


def solution(mesh):
    placed = (P("gz", "gy", None), P("gz", "gy", None))
    return jax.shard_map(
        per_device, mesh=mesh, in_specs=placed, out_specs=P("gz", "gy", None), check_vma=False
    )
```

```python
import functools

import jax
import jax.numpy as jnp
import numpy as np
from jax import lax
from jax.experimental import pallas as pl
from jax.experimental.pallas import tpu as pltpu
from jax.sharding import PartitionSpec as P

AXES = ("gz", "gy")


def angle(first, second, count):
    return 2.0 * np.pi / count * ((first * second) % count)


def x_table(count, replicas, devices):
    half = replicas // 2
    columns = count * half // devices
    device, part, column, x, side, pair = np.ix_(
        *(np.arange(s) for s in (devices, 2, columns, count, 2, half))
    )
    flat = device * columns + column
    theta = angle(flat // half, x, count)
    value = np.where(part == side, np.cos(theta), np.where(part == 0, np.sin(theta), -np.sin(theta)))
    value = value * (flat % half == pair)
    return value.reshape(devices * 2 * columns, count, replicas)


def x_kernel_table(count, replicas, devices):
    half = replicas // 2
    columns = count * half // devices
    lines = max(1, columns // half)
    device, part, line, x = np.ix_(*(np.arange(s) for s in (devices, 2, lines, count)))
    theta = angle(device * columns // half + line, x, count)
    value = np.where(part == 0, np.cos(theta), -np.sin(theta))
    return value.reshape(devices * 2 * lines, count)


def y_table(count, planes, rows):
    part, block, plane, row, new_plane, new_part, freq = np.ix_(
        *(np.arange(s) for s in (2, count // rows, planes, rows, planes, 2, count))
    )
    theta = angle(block * rows + row, freq, count)
    value = np.where(
        part == new_part, np.cos(theta), np.where(new_part == 0, np.sin(theta), -np.sin(theta))
    )
    value = value * (plane == new_plane)
    return value.reshape(2 * count * planes, planes * 2 * count)


def z_table(count, planes, columns, lines, group, wave):
    blocks = count // planes
    low, high, column, z_low, z_high, line = np.ix_(
        *(np.arange(s) for s in (planes, blocks, columns, planes, blocks, lines))
    )
    theta = angle(high * planes + low, z_high * planes + z_low, count)
    value = wave(theta) * (column // group == line)
    return value.reshape(count * columns, count * lines)


def refined(values, axis):
    before = np.roll(values, 1, axis)
    after = np.roll(values, -1, axis)
    after_two = np.roll(values, -2, axis)
    middle = (9.0 * (values + after) - (before + after_two)) / 16.0
    stacked = np.stack([values, middle], axis=axis + 1)
    shape = list(values.shape)
    shape[axis] = 2 * shape[axis]
    return stacked.reshape(shape)


def const(values):
    return jnp.asarray(np.asarray(values, np.float32))


def dot(left, right, dims=((1,), (0,))):
    return lax.dot_general(
        left, right, (dims, ((), ())), precision=lax.Precision.HIGH,
        preferred_element_type=jnp.float32,
    )


def extended(block, axis, dim):
    size = lax.axis_size(axis)
    forward = [(i, (i + 1) % size) for i in range(size)]
    backward = [(target, source) for source, target in forward]
    low = lax.ppermute(lax.slice_in_dim(block, block.shape[dim] - 1, None, axis=dim), axis, forward)
    high = lax.ppermute(lax.slice_in_dim(block, 0, 2, axis=dim), axis, backward)
    return jnp.concatenate([low, block, high], axis=dim)


def refine_rim(haloed, axis, count):
    centre = lax.slice_in_dim(haloed, 1, 1 + count, axis=axis)
    before = lax.slice_in_dim(haloed, 0, count, axis=axis)
    after = lax.slice_in_dim(haloed, 2, 2 + count, axis=axis)
    after_two = lax.slice_in_dim(haloed, 3, 3 + count, axis=axis)
    middle = (9.0 * (centre + after) - (before + after_two)) / 16.0
    stacked = jnp.stack([centre, middle], axis=axis + 1)
    shape = list(centre.shape)
    shape[axis] = 2 * count
    return stacked.reshape(shape)


def plain(charges, kernel):
    planes, rows, count = kernel.shape
    replicas = charges.shape[2] // count
    half = replicas // 2
    blocks_z, blocks_y = lax.axis_size("gz"), lax.axis_size("gy")
    devices = blocks_z * blocks_y
    place = planes * rows
    columns = count * half // devices
    lines = max(1, columns // half)
    table_x = x_table(count, replicas, devices)
    table_y = const(y_table(count, planes, rows))
    cos_z = const(z_table(count, planes, columns, columns, 1, np.cos))
    sin_z = const(z_table(count, planes, columns, columns, 1, np.sin))
    cos_k = const(z_table(count, planes, columns, lines, half, np.cos) / count**3)
    sin_k = const(z_table(count, planes, columns, lines, half, np.sin) / count**3)

    sent = dot(const(table_x.reshape(-1, count * replicas)), charges.reshape(place, -1), ((1,), (1,)))
    sent_k = dot(const(x_kernel_table(count, replicas, devices)), kernel.reshape(place, count), ((1,), (1,)))
    both = jnp.concatenate(
        [sent.reshape(devices, 2 * columns, place), sent_k.reshape(devices, 2 * lines, place)], axis=1
    )
    both = lax.all_to_all(both, AXES, split_axis=0, concat_axis=0, tiled=True)

    def by_y(block, width):
        block = block.reshape(blocks_z, blocks_y, 2, width, place).transpose(0, 3, 2, 1, 4)
        block = dot(block.reshape(blocks_z * width, 2 * blocks_y * place), table_y)
        block = block.reshape(blocks_z * width, planes, 2 * count).transpose(1, 0, 2)
        return block.reshape(count * width, 2 * count)

    def swap(values):
        return jnp.concatenate([values[:, count:], values[:, :count]], axis=1)

    sign = jnp.where(lax.broadcasted_iota(jnp.int32, (1, 2 * count), 1) < count, 1.0, -1.0)
    data = by_y(both[:, : 2 * columns], columns)
    green = by_y(both[:, 2 * columns :], lines)
    data = dot(cos_z, data) + sign * swap(dot(sin_z, data))
    green = dot(cos_k, green) + sign * swap(dot(sin_k, green))
    real, imag = green[:, :count], green[:, count:]
    data = data * jnp.concatenate([real, real], axis=1) + swap(data) * jnp.concatenate([-imag, imag], axis=1)
    data = dot(cos_z, data) - sign * swap(dot(sin_z, data))
    data = data.reshape(planes, blocks_z * columns, 2 * count).transpose(1, 0, 2)
    data = dot(data.reshape(blocks_z * columns, planes * 2 * count), table_y, ((1,), (1,)))
    data = data.reshape(blocks_z, columns, 2, blocks_y, place).transpose(0, 3, 2, 1, 4)
    data = lax.all_to_all(
        data.reshape(devices, 2 * columns, place), AXES, split_axis=0, concat_axis=0, tiled=True
    )
    fine_x = const(refined(table_x, 1).reshape(-1, 2 * count * replicas))
    result = dot(data.reshape(devices * 2 * columns, place), fine_x, ((0,), (0,)))
    result = result.reshape(planes, rows, 2 * count * replicas)
    result = extended(extended(result, "gz", 0), "gy", 1)
    result = refine_rim(result, 0, planes)
    return refine_rim(result, 1, rows)


LANES = 128
MESH = pl.DeviceIdType.MESH


def table(values):
    high = np.asarray(values, np.float32).astype(jnp.bfloat16)
    low = (np.asarray(values, np.float64) - high.astype(np.float64)).astype(jnp.bfloat16)
    return [jnp.asarray(high), jnp.asarray(low)]


def split(values):
    high = values.astype(jnp.bfloat16)
    return high, (values - high.astype(jnp.float32)).astype(jnp.bfloat16)


def mul(left, right, dims=((1,), (0,))):
    return lax.dot_general(left, right, (dims, ((), ())), preferred_element_type=jnp.float32)


def mul3(left, right, dims=((1,), (0,))):
    (a, b), (c, d) = left, right
    return mul(a, d, dims) + mul(b, c, dims) + mul(a, c, dims)


def exchange(blocks_z, blocks_y, x_ref, o_ref, send_sem, recv_sem, own_sem):
    devices = blocks_z * blocks_y
    me = lax.axis_index("gz") * blocks_y + lax.axis_index("gy")
    copies = []
    for step in sorted(range(1, devices), key=lambda s: abs(s - devices // 2)):
        other = lax.rem(me + step, devices)
        copy = pltpu.make_async_remote_copy(
            src_ref=x_ref.at[other], dst_ref=o_ref.at[me],
            send_sem=send_sem.at[step], recv_sem=recv_sem.at[step],
            device_id=(other // blocks_y, lax.rem(other, blocks_y)), device_id_type=MESH,
        )
        copy.start()
        copies.append(copy)
    own = pltpu.make_async_copy(x_ref.at[me], o_ref.at[me], own_sem)
    own.start()
    copies.append(own)
    return copies


def remote(source, target, sems, number, place):
    copy = pltpu.make_async_remote_copy(
        src_ref=source, dst_ref=target, send_sem=sems.at[0, number], recv_sem=sems.at[1, number],
        device_id=place, device_id_type=MESH,
    )
    copy.start()
    return copy


def main_kernel(sizes, *refs):
    columns, count, blocks_z, blocks_y, n_tables = sizes
    devices = blocks_z * blocks_y
    q_ref, k_ref = refs[0], refs[1]
    sources = refs[2 : 2 + n_tables]
    out = refs[2 + n_tables]
    tables = refs[3 + n_tables : 3 + 2 * n_tables]
    (sent, held, back, home, coarse, up, down, from_low, from_high,
     table_sem, send_a, recv_a, send_b, recv_b, own_sem, halo_sem) = refs[3 + 2 * n_tables :]
    loads = [pltpu.make_async_copy(s, t, table_sem.at[i]) for i, (s, t) in enumerate(zip(sources, tables))]
    for load in loads:
        load.start()
    gz, gy = lax.axis_index("gz"), lax.axis_index("gy")
    me = gz * blocks_y + gy
    barrier = pltpu.get_barrier_semaphore()
    for step in range(1, devices):
        other = lax.rem(me + step, devices)
        pl.semaphore_signal(
            barrier, inc=1, device_id=(other // blocks_y, lax.rem(other, blocks_y)), device_id_type=MESH
        )
    for load in loads[:4]:
        load.wait()
    table_x = (tables[0][...], tables[1][...])
    first_stage(2 * columns, q_ref, k_ref, table_x, (tables[2][...], tables[3][...]), sent)
    pl.semaphore_wait(barrier, devices - 1)
    copies = exchange(blocks_z, blocks_y, sent, held, send_a, recv_a, own_sem.at[0])
    for load in loads[4:]:
        load.wait()
    for copy in copies:
        copy.wait()
    pairs = [(tables[i][...], tables[i + 1][...]) for i in range(4, n_tables, 2)]
    middle_stage(columns, count, blocks_z, blocks_y, held, pairs, back)
    copies = exchange(blocks_z, blocks_y, back, home, send_b, recv_b, own_sem.at[1])
    for copy in copies:
        copy.wait()
    planes, rows, width = coarse.shape
    turned = jnp.transpose(home[...].reshape(width, LANES))
    made = mul3(split(turned), (tables[0][...], tables[1][...])).reshape(planes, rows, width)
    coarse[...] = made
    above = (lax.rem(gz + 1, blocks_z), gy)
    below = (lax.rem(gz + blocks_z - 1, blocks_z), gy)
    copies = [
        remote(coarse.at[pl.ds(planes - 1, 1)], out.at[pl.ds(0, 1), pl.ds(0, rows)], halo_sem, 0, above),
        remote(coarse.at[pl.ds(0, 2)], out.at[pl.ds(planes + 1, 2), pl.ds(0, rows)], halo_sem, 1, below),
    ]
    out[1 : planes + 1, :rows, :] = made
    for p in range(1, planes + 1):
        up[p : p + 1, :] = coarse[p - 1, rows - 1 : rows, :]
        down[2 * p : 2 * p + 2, :] = coarse[p - 1, 0:2, :]
    for copy in copies:
        copy.wait()
    for p in (0, planes + 1, planes + 2):
        up[p : p + 1, :] = out[p, rows - 1 : rows, :]
        down[2 * p : 2 * p + 2, :] = out[p, 0:2, :]
    above = (gz, lax.rem(gy + 1, blocks_y))
    below = (gz, lax.rem(gy + blocks_y - 1, blocks_y))
    copies = [remote(up, from_low, halo_sem, 2, above), remote(down, from_high, halo_sem, 3, below)]
    for copy in copies:
        copy.wait()
    empty = jnp.zeros((5, width), jnp.float32)
    for p in range(planes + 3):
        rim = [from_low[p : p + 1, :], from_high[2 * p : 2 * p + 2, :], empty]
        out[p, rows : rows + 8, :] = jnp.concatenate(rim, axis=0)


def first_stage(width, q_ref, k_ref, table_x, lines_x, o_ref):
    devices = o_ref.shape[0]
    dims = ((1,), (1,))
    sent = mul3(lines_x, split(k_ref[...]), dims)
    o_ref[:, width:, :] = sent.reshape(devices, 8, LANES)
    sent = mul3(table_x, split(q_ref[...]), dims)
    o_ref[:, :width, :] = sent.reshape(devices, width, LANES)


def middle_stage(columns, count, blocks_z, blocks_y, held, tables, o_ref):
    planes = count // blocks_z
    table_y, cos_z, sin_z, green_a, green_b = tables
    x_ref = held[...].reshape(blocks_z, blocks_y, *held.shape[1:])
    lane = lax.broadcasted_iota(jnp.int32, (1, LANES), 1)
    sign = jnp.where(lane < count, 1.0, -1.0)

    def swap(values):
        return pltpu.roll(values, count, 1)

    def lines_first(values):
        return jnp.concatenate([values[:, p * LANES : (p + 1) * LANES] for p in range(planes)], axis=0)

    data = jnp.concatenate(
        [
            x_ref[:, y, c * columns : (c + 1) * columns, :].reshape(blocks_z * columns, LANES)
            for c in range(2)
            for y in range(blocks_y)
        ],
        axis=1,
    )
    green = jnp.concatenate(
        [x_ref[:, y, 2 * columns :, :].reshape(blocks_z * 8, LANES) for y in range(blocks_y)], axis=1
    )
    data = lines_first(mul3(split(data), table_y))
    deep = blocks_y * LANES
    green = lines_first(mul3(split(green), tuple(t[:deep, :] for t in table_y)))
    data = split(data)
    data = mul3(cos_z, data) + sign * swap(mul3(sin_z, data))
    green = split(green)
    green = mul3(green_a, green) - sign * swap(mul3(green_b, green))
    other = swap(green)
    real = jnp.where(lane < count, green, other)
    imag = jnp.where(lane < count, -other, green)
    data = split(data * real + swap(data) * imag)
    data = mul3(cos_z, data) - sign * swap(mul3(sin_z, data))
    size = blocks_z * columns
    data = jnp.concatenate([data[p * size : (p + 1) * size, :] for p in range(planes)], axis=1)
    data = mul3(split(data), table_y, ((1,), (1,)))
    for c in range(2):
        pieces = [
            data[:, (c * blocks_y + y) * LANES : (c * blocks_y + y + 1) * LANES].reshape(
                blocks_z, 1, columns, LANES
            )
            for y in range(blocks_y)
        ]
        piece = jnp.concatenate(pieces, axis=1).reshape(blocks_z * blocks_y, columns, LANES)
        o_ref[:, c * columns : (c + 1) * columns, :] = piece


def refine_kernel(x_ref, r_ref, t_ref, o_ref):
    step = pl.program_id(0)
    near = x_ref[pl.ds(step, 4)].reshape(4 * x_ref.shape[1], x_ref.shape[2])
    high, low = split(near)
    fine = mul(r_ref[...], low) + mul(r_ref[...], high)
    high, low = split(fine)
    blocks = fine.shape[1] // LANES
    for b in range(blocks):
        def window(values):
            pieces = [(b + s) % blocks * LANES for s in (-1, 0, 1)]
            return jnp.concatenate([values[:, p : p + LANES] for p in pieces], axis=1)

        made = mul(window(low), t_ref[...]) + mul(window(high), t_ref[...])
        o_ref[:, :, 2 * b * LANES : 2 * (b + 1) * LANES] = made.reshape(2, -1, 2 * LANES)


def rim_table(count):
    made = np.zeros((2 * count, count + 3))
    for i in range(count):
        made[2 * i, i + 1] = 1.0
        made[2 * i + 1, i : i + 4] = np.array([-1.0, 9.0, 9.0, -1.0]) / 16.0
    return made


def refine(haloed, planes, rows, width, replicas):
    along_y = rim_table(rows)
    empty = np.zeros((2 * rows, 5))
    along_y = np.concatenate([along_y[:, 1 : rows + 1], along_y[:, :1], along_y[:, rows + 1 :], empty], axis=1)
    both = jnp.asarray(np.kron(rim_table(1), along_y), jnp.bfloat16)
    count = width // replicas
    spread = refined(np.eye(width).reshape(width, count, replicas), 1).reshape(width, 2 * width)
    spread = jnp.asarray(spread[: 3 * LANES, 2 * LANES : 4 * LANES], jnp.bfloat16)
    return pl.pallas_call(
        refine_kernel,
        grid=(planes,),
        out_shape=jax.ShapeDtypeStruct((2 * planes, 2 * rows, 2 * width), jnp.float32),
        in_specs=[
            pl.BlockSpec(haloed.shape, lambda i: (0, 0, 0)),
            pl.BlockSpec(both.shape, lambda i: (0, 0)),
            pl.BlockSpec(spread.shape, lambda i: (0, 0)),
        ],
        out_specs=pl.BlockSpec((2, 2 * rows, 2 * width), lambda i: (i, 0, 0)),
    )(haloed, both, spread)


def z_green_table(count, planes, columns, group, first, second):
    lines = max(1, columns // group)
    rows = []
    for wave in (first, second):
        made = z_table(count, planes, columns, lines, group, wave)
        rows.append(made.reshape(count * columns, count, lines))
    made = np.concatenate(rows, axis=2)
    made = np.pad(made, ((0, 0), (0, 0), (0, 8 - 2 * lines)))
    return made.reshape(count * columns, count * 8)


def per_device(charges, kernel):
    planes, rows, count = kernel.shape
    width = charges.shape[2]
    replicas = width // count
    half = replicas // 2
    blocks_z, blocks_y = lax.axis_size("gz"), lax.axis_size("gy")
    devices = blocks_z * blocks_y
    place = planes * rows
    columns = count * half // devices
    lines = max(1, columns // half)
    fits = place == LANES and 2 * count == LANES and columns % 8 == 0 and 2 * lines <= 8
    if not fits or LANES % replicas or width < 3 * LANES or rows % 8 or planes < 2:
        return plain(charges, kernel)
    table_x = table(x_table(count, replicas, devices).reshape(-1, width))
    lines_x = x_kernel_table(count, replicas, devices).reshape(devices, 2 * lines, count)
    lines_x = table(np.pad(lines_x, ((0, 0), (0, 8 - 2 * lines), (0, 0))).reshape(devices * 8, count))
    table_y = table(y_table(count, planes, rows))
    cos_z = table(z_table(count, planes, columns, columns, 1, np.cos))
    sin_z = table(z_table(count, planes, columns, columns, 1, np.sin))
    scale = 1.0 / count**3
    green_a = table(scale * z_green_table(count, planes, columns, half, np.cos, np.sin))
    green_b = table(scale * z_green_table(count, planes, columns, half, lambda t: -np.sin(t), np.cos))

    tables = [*table_x, *lines_x, *table_y, *cos_z, *sin_z, *green_a, *green_b]
    size = 2 * columns
    packed = -(-(planes + 3) // 8) * 8
    vmem = pl.BlockSpec(memory_space=pltpu.VMEM)
    block = lambda *shape: pltpu.VMEM(shape, jnp.float32)
    haloed = pl.pallas_call(
        functools.partial(main_kernel, (columns, count, blocks_z, blocks_y, len(tables))),
        out_shape=jax.ShapeDtypeStruct((planes + 3, rows + 8, width), jnp.float32),
        in_specs=[vmem, vmem] + [pl.BlockSpec(memory_space=pl.ANY)] * len(tables),
        out_specs=vmem,
        scratch_shapes=[
            *(pltpu.VMEM(t.shape, t.dtype) for t in tables),
            block(devices, size + 8, LANES), block(devices, size + 8, LANES),
            block(devices, size, LANES), block(devices, size, LANES),
            block(planes, rows, width),
            block(packed, width), block(2 * packed, width),
            block(packed, width), block(2 * packed, width),
            pltpu.SemaphoreType.DMA((len(tables),)),
            *(pltpu.SemaphoreType.DMA((devices,)) for _ in range(4)),
            pltpu.SemaphoreType.DMA((2,)),
            pltpu.SemaphoreType.DMA((2, 4)),
        ],
        compiler_params=pltpu.CompilerParams(
            collective_id=0, has_side_effects=True, vmem_limit_bytes=60 * 1024 * 1024
        ),
    )(charges.reshape(place, width), kernel.reshape(place, count), *tables)
    return refine(haloed, planes, rows, width, replicas)


def solution(mesh):
    placed = (P("gz", "gy", None), P("gz", "gy", None))
    return jax.shard_map(
        per_device, mesh=mesh, in_specs=placed, out_specs=P("gz", "gy", None), check_vma=False
    )
```

```python
import functools

import jax
import jax.numpy as jnp
import numpy as np
from jax import lax
from jax.experimental import pallas as pl
from jax.experimental.pallas import tpu as pltpu
from jax.sharding import PartitionSpec as P

AXES = ("gz", "gy")


def angle(first, second, count):
    return 2.0 * np.pi / count * ((first * second) % count)


def x_table(count, replicas, devices):
    half = replicas // 2
    columns = count * half // devices
    device, part, column, x, side, pair = np.ix_(
        *(np.arange(s) for s in (devices, 2, columns, count, 2, half))
    )
    flat = device * columns + column
    theta = angle(flat // half, x, count)
    value = np.where(part == side, np.cos(theta), np.where(part == 0, np.sin(theta), -np.sin(theta)))
    value = value * (flat % half == pair)
    return value.reshape(devices * 2 * columns, count, replicas)


def x_kernel_table(count, replicas, devices):
    half = replicas // 2
    columns = count * half // devices
    lines = max(1, columns // half)
    device, part, line, x = np.ix_(*(np.arange(s) for s in (devices, 2, lines, count)))
    theta = angle(device * columns // half + line, x, count)
    value = np.where(part == 0, np.cos(theta), -np.sin(theta))
    return value.reshape(devices * 2 * lines, count)


def y_table(count, planes, rows):
    part, block, plane, row, new_plane, new_part, freq = np.ix_(
        *(np.arange(s) for s in (2, count // rows, planes, rows, planes, 2, count))
    )
    theta = angle(block * rows + row, freq, count)
    value = np.where(
        part == new_part, np.cos(theta), np.where(new_part == 0, np.sin(theta), -np.sin(theta))
    )
    value = value * (plane == new_plane)
    return value.reshape(2 * count * planes, planes * 2 * count)


def z_table(count, planes, columns, lines, group, wave):
    blocks = count // planes
    low, high, column, z_low, z_high, line = np.ix_(
        *(np.arange(s) for s in (planes, blocks, columns, planes, blocks, lines))
    )
    theta = angle(high * planes + low, z_high * planes + z_low, count)
    value = wave(theta) * (column // group == line)
    return value.reshape(count * columns, count * lines)


def refined(values, axis):
    before = np.roll(values, 1, axis)
    after = np.roll(values, -1, axis)
    after_two = np.roll(values, -2, axis)
    middle = (9.0 * (values + after) - (before + after_two)) / 16.0
    stacked = np.stack([values, middle], axis=axis + 1)
    shape = list(values.shape)
    shape[axis] = 2 * shape[axis]
    return stacked.reshape(shape)


def const(values):
    return jnp.asarray(np.asarray(values, np.float32))


def dot(left, right, dims=((1,), (0,))):
    return lax.dot_general(
        left, right, (dims, ((), ())), precision=lax.Precision.HIGH,
        preferred_element_type=jnp.float32,
    )


def extended(block, axis, dim):
    size = lax.axis_size(axis)
    forward = [(i, (i + 1) % size) for i in range(size)]
    backward = [(target, source) for source, target in forward]
    low = lax.ppermute(lax.slice_in_dim(block, block.shape[dim] - 1, None, axis=dim), axis, forward)
    high = lax.ppermute(lax.slice_in_dim(block, 0, 2, axis=dim), axis, backward)
    return jnp.concatenate([low, block, high], axis=dim)


def refine_rim(haloed, axis, count):
    centre = lax.slice_in_dim(haloed, 1, 1 + count, axis=axis)
    before = lax.slice_in_dim(haloed, 0, count, axis=axis)
    after = lax.slice_in_dim(haloed, 2, 2 + count, axis=axis)
    after_two = lax.slice_in_dim(haloed, 3, 3 + count, axis=axis)
    middle = (9.0 * (centre + after) - (before + after_two)) / 16.0
    stacked = jnp.stack([centre, middle], axis=axis + 1)
    shape = list(centre.shape)
    shape[axis] = 2 * count
    return stacked.reshape(shape)


def plain(charges, kernel):
    planes, rows, count = kernel.shape
    replicas = charges.shape[2] // count
    half = replicas // 2
    blocks_z, blocks_y = lax.axis_size("gz"), lax.axis_size("gy")
    devices = blocks_z * blocks_y
    place = planes * rows
    columns = count * half // devices
    lines = max(1, columns // half)
    table_x = x_table(count, replicas, devices)
    table_y = const(y_table(count, planes, rows))
    cos_z = const(z_table(count, planes, columns, columns, 1, np.cos))
    sin_z = const(z_table(count, planes, columns, columns, 1, np.sin))
    cos_k = const(z_table(count, planes, columns, lines, half, np.cos) / count**3)
    sin_k = const(z_table(count, planes, columns, lines, half, np.sin) / count**3)

    sent = dot(const(table_x.reshape(-1, count * replicas)), charges.reshape(place, -1), ((1,), (1,)))
    sent_k = dot(const(x_kernel_table(count, replicas, devices)), kernel.reshape(place, count), ((1,), (1,)))
    both = jnp.concatenate(
        [sent.reshape(devices, 2 * columns, place), sent_k.reshape(devices, 2 * lines, place)], axis=1
    )
    both = lax.all_to_all(both, AXES, split_axis=0, concat_axis=0, tiled=True)

    def by_y(block, width):
        block = block.reshape(blocks_z, blocks_y, 2, width, place).transpose(0, 3, 2, 1, 4)
        block = dot(block.reshape(blocks_z * width, 2 * blocks_y * place), table_y)
        block = block.reshape(blocks_z * width, planes, 2 * count).transpose(1, 0, 2)
        return block.reshape(count * width, 2 * count)

    def swap(values):
        return jnp.concatenate([values[:, count:], values[:, :count]], axis=1)

    sign = jnp.where(lax.broadcasted_iota(jnp.int32, (1, 2 * count), 1) < count, 1.0, -1.0)
    data = by_y(both[:, : 2 * columns], columns)
    green = by_y(both[:, 2 * columns :], lines)
    data = dot(cos_z, data) + sign * swap(dot(sin_z, data))
    green = dot(cos_k, green) + sign * swap(dot(sin_k, green))
    real, imag = green[:, :count], green[:, count:]
    data = data * jnp.concatenate([real, real], axis=1) + swap(data) * jnp.concatenate([-imag, imag], axis=1)
    data = dot(cos_z, data) - sign * swap(dot(sin_z, data))
    data = data.reshape(planes, blocks_z * columns, 2 * count).transpose(1, 0, 2)
    data = dot(data.reshape(blocks_z * columns, planes * 2 * count), table_y, ((1,), (1,)))
    data = data.reshape(blocks_z, columns, 2, blocks_y, place).transpose(0, 3, 2, 1, 4)
    data = lax.all_to_all(
        data.reshape(devices, 2 * columns, place), AXES, split_axis=0, concat_axis=0, tiled=True
    )
    fine_x = const(refined(table_x, 1).reshape(-1, 2 * count * replicas))
    result = dot(data.reshape(devices * 2 * columns, place), fine_x, ((0,), (0,)))
    result = result.reshape(planes, rows, 2 * count * replicas)
    result = extended(extended(result, "gz", 0), "gy", 1)
    result = refine_rim(result, 0, planes)
    return refine_rim(result, 1, rows)


LANES = 128
MESH = pl.DeviceIdType.MESH


def table(values):
    high = np.asarray(values, np.float32).astype(jnp.bfloat16)
    low = (np.asarray(values, np.float64) - high.astype(np.float64)).astype(jnp.bfloat16)
    return [jnp.asarray(high), jnp.asarray(low)]


def split(values):
    high = values.astype(jnp.bfloat16)
    return high, (values - high.astype(jnp.float32)).astype(jnp.bfloat16)


def mul(left, right, dims=((1,), (0,))):
    return lax.dot_general(left, right, (dims, ((), ())), preferred_element_type=jnp.float32)


def mul3(left, right, dims=((1,), (0,))):
    (a, b), (c, d) = left, right
    return mul(a, d, dims) + mul(b, c, dims) + mul(a, c, dims)


GROUPS = 4
ORDER = (2, 3, 1, 0)


def send_group(blocks_z, blocks_y, offset, x_ref, o_ref, sems, own_sem):
    size = blocks_z * blocks_y // GROUPS
    me = lax.axis_index("gz") * blocks_y + lax.axis_index("gy")
    target = lax.rem(me // size + offset, GROUPS)
    copies = []
    for step in range(size):
        if offset == 0 and step == 0:
            copy = pltpu.make_async_copy(x_ref.at[me], o_ref.at[me], own_sem)
        else:
            other = target * size + lax.rem(lax.rem(me, size) + step, size)
            number = offset * size + step
            copy = pltpu.make_async_remote_copy(
                src_ref=x_ref.at[other], dst_ref=o_ref.at[me],
                send_sem=sems[0].at[number], recv_sem=sems[1].at[number],
                device_id=(other // blocks_y, lax.rem(other, blocks_y)), device_id_type=MESH,
            )
        copy.start()
        copies.append(copy)
    return copies


def remote(source, target, sems, number, place):
    copy = pltpu.make_async_remote_copy(
        src_ref=source, dst_ref=target, send_sem=sems.at[0, number], recv_sem=sems.at[1, number],
        device_id=place, device_id_type=MESH,
    )
    copy.start()
    return copy


def main_kernel(sizes, *refs):
    columns, count, blocks_z, blocks_y, n_tables = sizes
    devices = blocks_z * blocks_y
    q_ref, k_ref = refs[0], refs[1]
    sources = refs[2 : 2 + n_tables]
    out = refs[2 + n_tables]
    tables = refs[3 + n_tables : 3 + 2 * n_tables]
    (sent, held, back, home, coarse, up, down, from_low, from_high,
     table_sem, send_a, recv_a, send_b, recv_b, own_sem, halo_sem) = refs[3 + 2 * n_tables :]
    loads = [pltpu.make_async_copy(s, t, table_sem.at[i]) for i, (s, t) in enumerate(zip(sources, tables))]
    for load in loads:
        load.start()
    gz, gy = lax.axis_index("gz"), lax.axis_index("gy")
    me = gz * blocks_y + gy
    barrier = pltpu.get_barrier_semaphore()
    for step in range(1, devices):
        other = lax.rem(me + step, devices)
        pl.semaphore_signal(
            barrier, inc=1, device_id=(other // blocks_y, lax.rem(other, blocks_y)), device_id_type=MESH
        )
    for load in loads[:4]:
        load.wait()
    width = q_ref.shape[1]
    size = devices // GROUPS
    deep = size * 2 * columns
    green = mul3((tables[2][...], tables[3][...]), split(k_ref[...]), ((1,), (1,)))
    sent[:, 2 * columns :, :] = green.reshape(devices, 8, LANES)
    charges = split(q_ref[...])

    def table_rows(group):
        place = pl.ds(pl.multiple_of(group * deep, deep), deep)
        return tables[0][place, :], tables[1][place, :]

    copies = []
    for offset in ORDER:
        group = lax.rem(me // size + offset, GROUPS)
        made = mul3(table_rows(group), charges, ((1,), (1,)))
        sent[pl.ds(group * size, size), : 2 * columns, :] = made.reshape(size, 2 * columns, LANES)
        if not copies:
            pl.semaphore_wait(barrier, devices - 1)
        copies += send_group(blocks_z, blocks_y, offset, sent, held, (send_a, recv_a), own_sem.at[0])
    for load in loads[4:]:
        load.wait()
    for copy in copies:
        copy.wait()
    pairs = [(tables[i][...], tables[i + 1][...]) for i in range(4, n_tables, 2)]
    middle_stage(columns, count, blocks_z, blocks_y, held, pairs, back)
    copies = [
        send_group(blocks_z, blocks_y, offset, back, home, (send_b, recv_b), own_sem.at[1])
        for offset in ORDER
    ]
    planes, rows, _ = coarse.shape
    made = jnp.zeros((LANES, width), jnp.float32)
    for offset, group_copies in zip(ORDER, copies):
        for copy in group_copies:
            copy.wait()
        group = lax.rem(me // size + GROUPS - offset, GROUPS)
        turned = jnp.transpose(home[pl.ds(group * size, size)].reshape(deep, LANES))
        made += mul3(split(turned), table_rows(group))
    made = made.reshape(planes, rows, width)
    coarse[...] = made
    above = (lax.rem(gz + 1, blocks_z), gy)
    below = (lax.rem(gz + blocks_z - 1, blocks_z), gy)
    copies = [
        remote(coarse.at[pl.ds(planes - 1, 1)], out.at[pl.ds(0, 1), pl.ds(0, rows)], halo_sem, 0, above),
        remote(coarse.at[pl.ds(0, 2)], out.at[pl.ds(planes + 1, 2), pl.ds(0, rows)], halo_sem, 1, below),
    ]
    out[1 : planes + 1, :rows, :] = made
    for p in range(1, planes + 1):
        up[p : p + 1, :] = coarse[p - 1, rows - 1 : rows, :]
        down[2 * p : 2 * p + 2, :] = coarse[p - 1, 0:2, :]
    for copy in copies:
        copy.wait()
    for p in (0, planes + 1, planes + 2):
        up[p : p + 1, :] = out[p, rows - 1 : rows, :]
        down[2 * p : 2 * p + 2, :] = out[p, 0:2, :]
    above = (gz, lax.rem(gy + 1, blocks_y))
    below = (gz, lax.rem(gy + blocks_y - 1, blocks_y))
    copies = [remote(up, from_low, halo_sem, 2, above), remote(down, from_high, halo_sem, 3, below)]
    for copy in copies:
        copy.wait()
    empty = jnp.zeros((5, width), jnp.float32)
    for p in range(planes + 3):
        rim = [from_low[p : p + 1, :], from_high[2 * p : 2 * p + 2, :], empty]
        out[p, rows : rows + 8, :] = jnp.concatenate(rim, axis=0)


def middle_stage(columns, count, blocks_z, blocks_y, held, tables, o_ref):
    planes = count // blocks_z
    table_y, cos_z, sin_z, green_a, green_b = tables
    x_ref = held[...].reshape(blocks_z, blocks_y, *held.shape[1:])
    lane = lax.broadcasted_iota(jnp.int32, (1, LANES), 1)
    sign = jnp.where(lane < count, 1.0, -1.0)

    def swap(values):
        return pltpu.roll(values, count, 1)

    def lines_first(values):
        return jnp.concatenate([values[:, p * LANES : (p + 1) * LANES] for p in range(planes)], axis=0)

    data = jnp.concatenate(
        [
            x_ref[:, y, c * columns : (c + 1) * columns, :].reshape(blocks_z * columns, LANES)
            for c in range(2)
            for y in range(blocks_y)
        ],
        axis=1,
    )
    green = jnp.concatenate(
        [x_ref[:, y, 2 * columns :, :].reshape(blocks_z * 8, LANES) for y in range(blocks_y)], axis=1
    )
    data = lines_first(mul3(split(data), table_y))
    deep = blocks_y * LANES
    green = lines_first(mul3(split(green), tuple(t[:deep, :] for t in table_y)))
    green = split(green)
    green = mul3(green_a, green) - sign * swap(mul3(green_b, green))
    half = cos_z[0].shape[0] // count

    def parts(values):
        values = values.reshape(count, columns, LANES)
        return [
            values[:, m : m + half, :].reshape(count * half, LANES) for m in range(0, columns, half)
        ]

    made = []
    for part, factor in zip(parts(data), parts(green)):
        part = split(part)
        part = mul3(cos_z, part) + sign * swap(mul3(sin_z, part))
        other = swap(factor)
        real = jnp.where(lane < count, factor, other)
        imag = jnp.where(lane < count, -other, factor)
        part = split(part * real + swap(part) * imag)
        part = mul3(cos_z, part) - sign * swap(mul3(sin_z, part))
        made.append(part.reshape(count, half, LANES))
    data = jnp.concatenate(made, axis=1).reshape(count * columns, LANES)
    size = blocks_z * columns
    data = jnp.concatenate([data[p * size : (p + 1) * size, :] for p in range(planes)], axis=1)
    data = mul3(split(data), table_y, ((1,), (1,)))
    for c in range(2):
        pieces = [
            data[:, (c * blocks_y + y) * LANES : (c * blocks_y + y + 1) * LANES].reshape(
                blocks_z, 1, columns, LANES
            )
            for y in range(blocks_y)
        ]
        piece = jnp.concatenate(pieces, axis=1).reshape(blocks_z * blocks_y, columns, LANES)
        o_ref[:, c * columns : (c + 1) * columns, :] = piece


def refine_kernel(x_ref, r_ref, t_ref, o_ref):
    step = pl.program_id(0)
    near = x_ref[pl.ds(step, 4)].reshape(4 * x_ref.shape[1], x_ref.shape[2])
    high, low = split(near)
    fine = mul(r_ref[...], low) + mul(r_ref[...], high)
    high, low = split(fine)
    blocks = fine.shape[1] // LANES
    def windows(values):
        made = []
        for b in range(blocks):
            pieces = [(b + s) % blocks * LANES for s in (-1, 0, 1)]
            made.append(jnp.concatenate([values[:, p : p + LANES] for p in pieces], axis=1))
        return jnp.concatenate(made, axis=0)

    made = mul(windows(low), t_ref[...]) + mul(windows(high), t_ref[...])
    for b in range(blocks):
        piece = made[b * fine.shape[0] : (b + 1) * fine.shape[0], :]
        o_ref[:, :, 2 * b * LANES : 2 * (b + 1) * LANES] = piece.reshape(2, -1, 2 * LANES)


def rim_table(count):
    made = np.zeros((2 * count, count + 3))
    for i in range(count):
        made[2 * i, i + 1] = 1.0
        made[2 * i + 1, i : i + 4] = np.array([-1.0, 9.0, 9.0, -1.0]) / 16.0
    return made


def refine(haloed, planes, rows, width, replicas):
    along_y = rim_table(rows)
    empty = np.zeros((2 * rows, 5))
    along_y = np.concatenate([along_y[:, 1 : rows + 1], along_y[:, :1], along_y[:, rows + 1 :], empty], axis=1)
    both = jnp.asarray(np.kron(rim_table(1), along_y), jnp.bfloat16)
    count = width // replicas
    spread = refined(np.eye(width).reshape(width, count, replicas), 1).reshape(width, 2 * width)
    spread = jnp.asarray(spread[: 3 * LANES, 2 * LANES : 4 * LANES], jnp.bfloat16)
    return pl.pallas_call(
        refine_kernel,
        grid=(planes,),
        out_shape=jax.ShapeDtypeStruct((2 * planes, 2 * rows, 2 * width), jnp.float32),
        in_specs=[
            pl.BlockSpec(haloed.shape, lambda i: (0, 0, 0)),
            pl.BlockSpec(both.shape, lambda i: (0, 0)),
            pl.BlockSpec(spread.shape, lambda i: (0, 0)),
        ],
        out_specs=pl.BlockSpec((2, 2 * rows, 2 * width), lambda i: (i, 0, 0)),
    )(haloed, both, spread)


def z_green_table(count, planes, columns, group, first, second):
    lines = max(1, columns // group)
    rows = []
    for wave in (first, second):
        made = z_table(count, planes, columns, lines, group, wave)
        rows.append(made.reshape(count * columns, count, lines))
    made = np.concatenate(rows, axis=2)
    made = np.pad(made, ((0, 0), (0, 0), (0, 8 - 2 * lines)))
    return made.reshape(count * columns, count * 8)


def per_device(charges, kernel):
    planes, rows, count = kernel.shape
    width = charges.shape[2]
    replicas = width // count
    half = replicas // 2
    blocks_z, blocks_y = lax.axis_size("gz"), lax.axis_size("gy")
    devices = blocks_z * blocks_y
    place = planes * rows
    columns = count * half // devices
    lines = max(1, columns // half)
    fits = place == LANES and 2 * count == LANES and columns % 8 == 0 and 2 * lines <= 8
    if not fits or LANES % replicas or width < 3 * LANES or rows % 8 or planes < 2 \
            or devices % GROUPS or half % 8 or columns % half:
        return plain(charges, kernel)
    table_x = table(x_table(count, replicas, devices).reshape(-1, width))
    lines_x = x_kernel_table(count, replicas, devices).reshape(devices, 2 * lines, count)
    lines_x = table(np.pad(lines_x, ((0, 0), (0, 8 - 2 * lines), (0, 0))).reshape(devices * 8, count))
    table_y = table(y_table(count, planes, rows))
    cos_z = table(z_table(count, planes, half, half, 1, np.cos))
    sin_z = table(z_table(count, planes, half, half, 1, np.sin))
    scale = 1.0 / count**3
    green_a = table(scale * z_green_table(count, planes, columns, half, np.cos, np.sin))
    green_b = table(scale * z_green_table(count, planes, columns, half, lambda t: -np.sin(t), np.cos))

    tables = [*table_x, *lines_x, *table_y, *cos_z, *sin_z, *green_a, *green_b]
    size = 2 * columns
    packed = -(-(planes + 3) // 8) * 8
    vmem = pl.BlockSpec(memory_space=pltpu.VMEM)
    block = lambda *shape: pltpu.VMEM(shape, jnp.float32)
    haloed = pl.pallas_call(
        functools.partial(main_kernel, (columns, count, blocks_z, blocks_y, len(tables))),
        out_shape=jax.ShapeDtypeStruct((planes + 3, rows + 8, width), jnp.float32),
        in_specs=[vmem, vmem] + [pl.BlockSpec(memory_space=pl.ANY)] * len(tables),
        out_specs=vmem,
        scratch_shapes=[
            *(pltpu.VMEM(t.shape, t.dtype) for t in tables),
            block(devices, size + 8, LANES), block(devices, size + 8, LANES),
            block(devices, size, LANES), block(devices, size, LANES),
            block(planes, rows, width),
            block(packed, width), block(2 * packed, width),
            block(packed, width), block(2 * packed, width),
            pltpu.SemaphoreType.DMA((len(tables),)),
            *(pltpu.SemaphoreType.DMA((devices,)) for _ in range(4)),
            pltpu.SemaphoreType.DMA((2,)),
            pltpu.SemaphoreType.DMA((2, 4)),
        ],
        compiler_params=pltpu.CompilerParams(
            collective_id=0, has_side_effects=True, vmem_limit_bytes=60 * 1024 * 1024
        ),
    )(charges.reshape(place, width), kernel.reshape(place, count), *tables)
    return refine(haloed, planes, rows, width, replicas)


def solution(mesh):
    placed = (P("gz", "gy", None), P("gz", "gy", None))
    return jax.shard_map(
        per_device, mesh=mesh, in_specs=placed, out_specs=P("gz", "gy", None), check_vma=False
    )
```
